768 devices in a mesh: band: 24 (over z_hi, y), slab: 32 (over x, z_lo, core).
Axes of the slice: x: 4, y: 8, z: 12 (z_hi: 3, z_lo: 4; z = z_hi * 4 + z_lo), core: 2. Of those that a mesh axis runs over, the one named last changes fastest.
Arguments:
- coefficients: float32 [48, 96, 96, 192], P('band', 'slab'), may hold values from -6 to 6
- occupation: int32 [48], P('band'), may hold values from 1 to 2
- pencil_reach: int32 [96, 96], P('slab'), may hold values from -1 to 47
- external: float32 [192, 192, 192], P(None, 'slab'), may hold values from -3 to 3
Outputs:
- applied: float32 [48, 96, 96, 192], P('band', 'slab')
- potential: float32 [192, 192, 192], P(None, 'slab')
The draws below stay inside these ranges and needn't reach their ends.
All inputs are finite; a program needn't handle non-finite values.
Results may differ from the reference program's by a relative error of at most 0.00011.
Values sent between devices are 32-bit elements; how exact they have to be, the bound alone decides.
No kernel may reach another device: no remote copies, remote signals or barrier semaphores. Data moves between devices by JAX's collectives and lax.ppermute only.
A program may use at most 32 MiB of HBM per device.

```python
import jax
import jax.numpy as jnp
from jax import lax

NW = 96
NG = 192
BANDS = 48


def draw_pencil_reach(key, part):
    halfway = NW // 2
    key_radius = jax.random.fold_in(key, 11)
    key_jitter = jax.random.fold_in(key, 23)
    radius_sq = jax.random.randint(key_radius, (), (halfway - 1) * (halfway - 1), halfway * halfway, dtype=jnp.int32)
    indices = jnp.arange(NW, dtype=jnp.int32)
    frequencies = jnp.where(indices < halfway, indices, indices - NW)
    planar = frequencies[:, None] * frequencies[:, None] + frequencies[None, :] * frequencies[None, :]
    offsets = jnp.arange(halfway + 1, dtype=jnp.int32)
    inside = planar[:, :, None] + offsets[None, None, :] * offsets[None, None, :] <= radius_sq
    extent = jnp.sum(inside.astype(jnp.int32), axis=2) - 1
    jitter = jax.random.randint(key_jitter, (NW, NW), 0, 2, dtype=jnp.int32)
    jitter = jnp.where(planar == 0, 0, jitter)
    return jnp.maximum(extent - jitter, -1)


def place_ends(values, key, smallest, largest):
    shape = values.shape
    index_at = [jax.random.randint(jax.random.fold_in(key, axis), (), 0, shape[axis]) for axis in range(len(shape))]
    values = values.at[tuple(index_at)].set(smallest)
    longest = shape.index(max(shape))
    index_at[longest] = (index_at[longest] + 1) % shape[longest]
    return values.at[tuple(index_at)].set(largest)


def block_levels(rng, dims, shards, least, high):
    level, own = 1.0, jax.random.fold_in(rng, 6)
    for dim, shards_of in shards:
        heights = jnp.exp(jax.random.uniform(jax.random.fold_in(own, dim), (shards_of,), jnp.float32, least / len(shards), high / len(shards)))
        level = level * jnp.repeat(heights, dims[dim] // shards_of).reshape([-1 if axis == dim else 1 for axis in range(len(dims))])
    return level


def centred(key, shape, deviation, most, shards=(), kind=jnp.bfloat16):
    result = jax.random.normal(key, shape, jnp.float32) * deviation
    if len(shards) > 0:
        result = block_levels(key, shape, shards, -0.22, 0.18) * result
    return jnp.clip(result, min=-most, max=most).astype(kind)


def setup_inputs(seed: int = 0) -> dict:
    keys = jax.random.split(jax.random.key(seed), 5)
    coefficients = centred(keys[0], (BANDS, NW, NW, 2 * NW), 1.0, 6.0, ((0, 24), (1, 32)), jnp.float32)
    occupation = place_ends(jax.random.randint(keys[1], (BANDS,), 1, 3), jax.random.fold_in(keys[1], 1), 1, 2).astype(jnp.int32)
    pencil_reach = draw_pencil_reach(jax.random.fold_in(keys[4], 71), 0)
    external = centred(keys[3], (NG, NG, NG), 0.5, 3.0, ((1, 32),), jnp.float32)
    return dict(coefficients=coefficients, occupation=occupation, pencil_reach=pencil_reach, external=external)


KINETIC = 0.0005
SLATER = 0.9847


def frequency(length):
    indices = jnp.arange(length, dtype=jnp.int32)
    return jnp.where(indices < length // 2, indices, indices - length)


def embed_grid(values):
    halfway = NW // 2
    for dimension in range(3):
        lower = lax.slice_in_dim(values, 0, halfway, axis=dimension)
        upper = lax.slice_in_dim(values, halfway, NW, axis=dimension)
        padding_shape = list(values.shape)
        padding_shape[dimension] = NG - NW
        values = jnp.concatenate([lower, jnp.zeros(padding_shape, values.dtype), upper], axis=dimension)
    return values


def extract_grid(values):
    halfway = NW // 2
    for dimension in range(3):
        lower = lax.slice_in_dim(values, 0, halfway, axis=dimension)
        upper = lax.slice_in_dim(values, NG - halfway, NG, axis=dimension)
        values = jnp.concatenate([lower, upper], axis=dimension)
    return values


def to_real(coefficient, sphere):
    real_part = coefficient[..., :NW] * sphere
    imag_part = coefficient[..., NW:] * sphere
    spectrum = lax.complex(real_part, imag_part)
    return jnp.fft.ifftn(embed_grid(spectrum)) * (NG ** 3 / NW ** 1.5)


def reference(coefficients, occupation, pencil_reach, external):
    wavenumbers = frequency(NW)
    sphere = (jnp.abs(wavenumbers)[None, None, :] <= pencil_reach[:, :, None]).astype(jnp.float32)
    weights = occupation.astype(jnp.float32) / BANDS

    def add_band(running, members):
        coefficient, weight = members
        wavefield = to_real(coefficient, sphere)
        squares = jnp.real(wavefield) * jnp.real(wavefield) + jnp.imag(wavefield) * jnp.imag(wavefield)
        return running + weight * squares, None

    density, _ = lax.scan(add_band, jnp.zeros((NG, NG, NG), jnp.float32), (coefficients, weights))
    potential_xyz = jnp.transpose(external, (0, 2, 1)) - SLATER * jnp.cbrt(density)
    squared = (wavenumbers * wavenumbers).astype(jnp.float32)
    kinetic = KINETIC * (squared[:, None, None] + squared[None, :, None] + squared[None, None, :])

    def apply_band(coefficient):
        wavefield = to_real(coefficient, sphere)
        returned = extract_grid(jnp.fft.fftn(wavefield * potential_xyz)) * (NW ** 1.5 / NG ** 3)
        real_out = sphere * (kinetic * (coefficient[..., :NW] * sphere) + jnp.real(returned))
        imag_out = sphere * (kinetic * (coefficient[..., NW:] * sphere) + jnp.imag(returned))
        return jnp.concatenate([real_out, imag_out], axis=-1)

    applied = lax.map(apply_band, coefficients)
    return applied, jnp.transpose(potential_xyz, (0, 2, 1))
```

```python
import jax
import jax.numpy as jnp
import numpy as np
from jax import lax
from jax.sharding import Mesh
from jax.sharding import PartitionSpec as P

BAND = ("zh", "y")
KINETIC = 0.0005
SLATER = 0.9847
HALVES = 2
LANES = 128


def frequency(length):
    indices = np.arange(length)
    return np.where(indices < length // 2, indices, indices - length)


def inverse_table(length, extent):
    phases = np.arange(extent)[:, None] * frequency(length)[None, :] % extent
    angles = phases * (2.0 * np.pi / extent)
    factor = length ** (-0.5)
    cosine, sine = np.cos(angles) * factor, np.sin(angles) * factor
    table = np.stack([np.stack([cosine, -sine], 1), np.stack([sine, cosine], 1)], 0)
    return table.astype(np.float32)


def forward_table(length, extent):
    phases = frequency(length)[:, None] * np.arange(extent)[None, :] % extent
    angles = phases * (2.0 * np.pi / extent)
    factor = length**0.5 / extent
    cosine, sine = np.cos(angles) * factor, np.sin(angles) * factor
    table = np.stack([np.stack([cosine, sine], 1), np.stack([-sine, cosine], 1)], 0)
    return table.astype(np.float32)


def contract(form, left, right):
    return jnp.einsum(form, left, right, precision=lax.Precision.HIGH)


def exchange_slab(rows):
    shape = rows.shape
    packed = rows.reshape(-1, 1, LANES)
    arrived = lax.all_to_all(packed, "slab", 0, 0, tiled=True)
    return arrived.reshape(shape)


def sum_by_permutes(blocks, axis):
    size = lax.axis_size(axis)
    index = lax.axis_index(axis)
    total = lax.dynamic_index_in_dim(blocks, index, 0, keepdims=False)
    for step in (4, 3, 5, 2, 6, 1, 7):
        piece = lax.dynamic_index_in_dim(blocks, (index + step) % size, 0, keepdims=False)
        total = total + lax.ppermute(piece, axis, [(i, (i + step) % size) for i in range(size)])
    return total


def sum_in_order(own, axis):
    index = lax.axis_index(axis)
    one_back = lax.ppermute(own, axis, [(0, 1), (1, 2), (2, 0)])
    two_back = lax.ppermute(own, axis, [(0, 2), (1, 0), (2, 1)])
    first = jnp.where(index == 2, two_back, jnp.where(index == 1, one_back, own))
    second = jnp.where(index == 2, one_back, jnp.where(index == 1, own, two_back))
    third = jnp.where(index == 2, own, jnp.where(index == 1, two_back, one_back))
    return (first + second) + third


def packed_rows(flat):
    members = lax.axis_size("y")
    dense = flat.reshape(-1, LANES)
    each = -(-dense.shape[0] // (members * 8)) * 8
    return jnp.pad(dense, ((0, members * each - dense.shape[0]), (0, 0)))


def shards(coefficients, occupation, pencil_reach, external):
    nbands, planes, width, doubled = coefficients.shape
    points = 2 * width
    slabs = lax.axis_size("slab")
    layers = points // slabs
    part = layers // HALVES
    groups = lax.axis_size("zh") * lax.axis_size("y")
    inverse = inverse_table(width, points)
    forward = forward_table(width, points)
    waves = frequency(width)
    weights = occupation.astype(jnp.float32) / (nbands * groups)

    reach2 = np.abs(np.concatenate([waves, waves])).astype(np.int32)
    sphere = (reach2[None, None, :] <= pencil_reach[:, :, None]).astype(jnp.float32)
    masked = coefficients * sphere[None]
    flat_masked = masked.reshape(nbands * planes * width, doubled)

    def by_half(table, axis):
        shape = table.shape
        return table.reshape(*shape[:axis], slabs, HALVES, part, *shape[axis + 1 :])

    inverse_z = by_half(inverse, 1).transpose(2, 1, 3, 0, 4, 5)
    inverse_z = inverse_z.reshape(HALVES, slabs * part * 2, doubled)
    forward_z = by_half(forward, 3).transpose(4, 3, 5, 2, 0, 1)
    forward_z = forward_z.reshape(HALVES, slabs * part * 2, doubled)
    ext = external.transpose(1, 0, 2).reshape(HALVES, part * points, points)
    member = lax.axis_index("y")

    outgoing = [contract("nk,rk->nr", inverse_z[h], flat_masked) for h in range(HALVES)]
    arrived = []
    for h in range(HALVES):
        rows = outgoing[h].reshape(slabs, part * 2 * nbands * planes * width)
        with jax.named_scope(f"inward{h}"):
            arrived.append(exchange_slab(rows))

    fields, partials = [], []
    for h in range(HALVES):
        if h > 0:
            arrived[h], _ = lax.optimization_barrier((arrived[h], partials[h - 1]))
        blocks = arrived[h].reshape(slabs, part, 2, nbands, planes, width)
        columns = blocks.transpose(3, 0, 4, 1, 2, 5).reshape(nbands, width, part, 2, width)
        spread = contract("bkzcg,oycg->bkzoy", columns, inverse)
        field = contract("bkzcy,oxck->bxzoy", spread, inverse)
        fields.append(field)
        squares = jnp.sum(field * field, axis=3)
        total = sum(weights[b] * squares[b] for b in range(nbands))
        partials.append(packed_rows(total.transpose(1, 0, 2).reshape(part * points, points)))

    potentials = []
    for h in range(HALVES):
        packed = partials[h]
        each = packed.shape[0] // lax.axis_size("y")
        blocks = packed.reshape(-1, each, LANES)
        if h == 0:
            own = sum_by_permutes(blocks, "y")
        else:
            own = jnp.sum(lax.all_to_all(blocks, "y", 0, 0, tiled=True), axis=0)
        with jax.named_scope(f"across{h}"):
            density = sum_in_order(own, "zh")
        own_external = lax.dynamic_slice_in_dim(packed_rows(ext[h]), member * each, each, 0)
        own_potential = own_external - SLATER * jnp.cbrt(density)
        with jax.named_scope(f"gather{h}"):
            gathered = lax.all_gather(own_potential, "y", axis=0, tiled=True)
        gathered = gathered[: part * points * points // LANES]
        potentials.append(gathered.reshape(part, points, points))

    returned = 0.0
    for h in range(HALVES):
        local = potentials[h].transpose(1, 0, 2)
        product = fields[h] * local[None, :, :, None, :]
        back_x = contract("bxzcy,okcx->bkzoy", product, forward)
        back_y = contract("bkzcy,ogcy->bkzog", back_x, forward)
        blocks = back_y.reshape(nbands, slabs, planes, part, 2, width)
        rows = blocks.transpose(1, 3, 4, 0, 2, 5).reshape(slabs, -1)
        with jax.named_scope(f"outward{h}"):
            home = exchange_slab(rows)
        home = home.reshape(slabs * part * 2, nbands * planes * width)
        returned = returned + contract("nr,nk->rk", home, forward_z[h])

    plane_index = lax.axis_index("slab") * planes + jnp.arange(planes, dtype=jnp.int32)
    plane_freq = jnp.where(plane_index < width // 2, plane_index, plane_index - width)
    plane_sq = (plane_freq * plane_freq).astype(jnp.float32)
    wave_sq = (waves * waves).astype(np.float32)
    both_sq = np.concatenate([wave_sq, wave_sq])
    kinetic = KINETIC * (plane_sq[:, None, None] + wave_sq[None, :, None] + both_sq[None, None, :])
    returned = returned.reshape(nbands, planes, width, doubled)
    applied = sphere[None] * (kinetic[None] * masked + returned)
    potential = jnp.concatenate(potentials, axis=0).transpose(1, 0, 2)
    return applied, potential


def solution(mesh):
    finer = Mesh(mesh.devices.reshape(3, 8, mesh.shape["slab"]), ("zh", "y", "slab"))
    return jax.shard_map(
        shards,
        mesh=finer,
        in_specs=(P(BAND, "slab", None, None), P(BAND), P("slab", None), P(None, "slab", None)),
        out_specs=(P(BAND, "slab", None, None), P(None, "slab", None)),
        check_vma=False,
    )
```

```python
import jax
import jax.numpy as jnp
import numpy as np
from jax import lax
from jax.sharding import Mesh
from jax.sharding import PartitionSpec as P

BAND = ("zh", "y")
KINETIC = 0.0005
SLATER = 0.9847
HALVES = 2
LANES = 128


def frequency(length):
    indices = np.arange(length)
    return np.where(indices < length // 2, indices, indices - length)


def inverse_table(length, extent):
    phases = np.arange(extent)[:, None] * frequency(length)[None, :] % extent
    angles = phases * (2.0 * np.pi / extent)
    factor = length ** (-0.5)
    cosine, sine = np.cos(angles) * factor, np.sin(angles) * factor
    table = np.stack([np.stack([cosine, -sine], 1), np.stack([sine, cosine], 1)], 0)
    return table.astype(np.float32)


def forward_table(length, extent):
    phases = frequency(length)[:, None] * np.arange(extent)[None, :] % extent
    angles = phases * (2.0 * np.pi / extent)
    factor = length**0.5 / extent
    cosine, sine = np.cos(angles) * factor, np.sin(angles) * factor
    table = np.stack([np.stack([cosine, sine], 1), np.stack([-sine, cosine], 1)], 0)
    return table.astype(np.float32)


def contract(form, left, right, precision=lax.Precision.HIGHEST):
    return jnp.einsum(form, left, right, precision=precision)


def exchange_slab(rows):
    shape = rows.shape
    packed = rows.reshape(-1, 1, LANES)
    arrived = lax.all_to_all(packed, "slab", 0, 0, tiled=True)
    return arrived.reshape(shape)


def shards(coefficients, occupation, pencil_reach, external):
    nbands, planes, width, doubled = coefficients.shape
    points = 2 * width
    slabs = lax.axis_size("slab")
    layers = points // slabs
    part = layers // HALVES
    groups = lax.axis_size("zh") * lax.axis_size("y")
    inverse = inverse_table(width, points)
    forward = forward_table(width, points)
    waves = frequency(width)
    weights = occupation.astype(jnp.float32) / (nbands * groups)

    reach2 = np.abs(np.concatenate([waves, waves])).astype(np.int32)
    sphere = (reach2[None, None, :] <= pencil_reach[:, :, None]).astype(jnp.float32)
    masked = coefficients * sphere[None]
    flat_masked = masked.reshape(nbands * planes * width, doubled)

    def by_half(table, axis):
        shape = table.shape
        return table.reshape(*shape[:axis], slabs, HALVES, part, *shape[axis + 1 :])

    inverse_z = by_half(inverse, 1).transpose(2, 1, 3, 0, 4, 5)
    inverse_z = inverse_z.reshape(HALVES, slabs * part * 2, doubled)
    forward_z = by_half(forward, 3).transpose(4, 3, 5, 2, 0, 1)
    forward_z = forward_z.reshape(HALVES, slabs * part * 2, doubled)

    outgoing = [contract("nk,rk->nr", inverse_z[h], flat_masked) for h in range(HALVES)]
    arrived = []
    for h in range(HALVES):
        rows = outgoing[h].reshape(slabs, part * 2 * nbands * planes * width)
        with jax.named_scope(f"inward{h}"):
            arrived.append(exchange_slab(rows))

    fields, partials = [], []
    for h in range(HALVES):
        if h > 0:
            arrived[h], _ = lax.optimization_barrier((arrived[h], partials[h - 1]))
        blocks = arrived[h].reshape(slabs, part, 2, nbands, planes, width)
        columns = blocks.transpose(3, 0, 4, 1, 2, 5).reshape(nbands, width, part, 2, width)
        spread = contract("bkzcg,oycg->bkzoy", columns, inverse)
        field = contract("bkzcy,oxck->bxzoy", spread, inverse, lax.Precision.HIGH)
        fields.append(field)
        squares = jnp.sum(field * field, axis=3)
        total = sum(weights[b] * squares[b] for b in range(nbands))
        partials.append(total.transpose(1, 0, 2).reshape(-1, LANES))

    members = lax.axis_size("y")
    packed = jnp.concatenate(partials, axis=0)
    blocks = packed.reshape(members, -1, LANES)
    own = jnp.sum(lax.all_to_all(blocks, "y", 0, 0, tiled=True), axis=0)
    copies = jnp.broadcast_to(own[None], (lax.axis_size("zh"), *own.shape))
    density = jnp.sum(lax.all_to_all(copies, "zh", 0, 0, tiled=True), axis=0)
    share = layers * points // members
    ext = external.transpose(1, 0, 2).reshape(layers * points, points)
    own_external = lax.dynamic_slice_in_dim(ext, lax.axis_index("y") * share, share, 0)
    own_potential = own_external.reshape(own.shape) - SLATER * jnp.cbrt(density)
    gathered = lax.all_gather(own_potential, "y", axis=0, tiled=True)
    potential = gathered.reshape(layers, points, points)

    returned = 0.0
    for h in range(HALVES):
        local = potential[h * part : (h + 1) * part].transpose(1, 0, 2)
        product = fields[h] * local[None, :, :, None, :]
        back_x = contract("bxzcy,okcx->bkzoy", product, forward, lax.Precision.HIGH)
        back_y = contract("bkzcy,ogcy->bkzog", back_x, forward)
        blocks = back_y.reshape(nbands, slabs, planes, part, 2, width)
        rows = blocks.transpose(1, 3, 4, 0, 2, 5).reshape(slabs, -1)
        with jax.named_scope(f"outward{h}"):
            home = exchange_slab(rows)
        home = home.reshape(slabs * part * 2, nbands * planes * width)
        returned = returned + contract("nr,nk->rk", home, forward_z[h])

    plane_index = lax.axis_index("slab") * planes + jnp.arange(planes, dtype=jnp.int32)
    plane_freq = jnp.where(plane_index < width // 2, plane_index, plane_index - width)
    plane_sq = (plane_freq * plane_freq).astype(jnp.float32)
    wave_sq = (waves * waves).astype(np.float32)
    both_sq = np.concatenate([wave_sq, wave_sq])
    kinetic = KINETIC * (plane_sq[:, None, None] + wave_sq[None, :, None] + both_sq[None, None, :])
    returned = returned.reshape(nbands, planes, width, doubled)
    applied = sphere[None] * (kinetic[None] * masked + returned)
    return applied, potential.transpose(1, 0, 2)


def solution(mesh):
    finer = Mesh(mesh.devices.reshape(3, 8, mesh.shape["slab"]), ("zh", "y", "slab"))
    return jax.shard_map(
        shards,
        mesh=finer,
        in_specs=(P(BAND, "slab", None, None), P(BAND), P("slab", None), P(None, "slab", None)),
        out_specs=(P(BAND, "slab", None, None), P(None, "slab", None)),
        check_vma=False,
    )
```

```python
import jax
import jax.numpy as jnp
import numpy as np
from jax import lax
from jax.sharding import Mesh
from jax.sharding import PartitionSpec as P

BAND = ("zh", "y")
KINETIC = 0.0005
SLATER = 0.9847
HALVES = 2
LANES = 128


def frequency(length):
    indices = np.arange(length)
    return np.where(indices < length // 2, indices, indices - length)


def inverse_table(length, extent):
    phases = np.arange(extent)[:, None] * frequency(length)[None, :] % extent
    angles = phases * (2.0 * np.pi / extent)
    factor = length ** (-0.5)
    cosine, sine = np.cos(angles) * factor, np.sin(angles) * factor
    table = np.stack([np.stack([cosine, -sine], 1), np.stack([sine, cosine], 1)], 0)
    return table.astype(np.float32)


def forward_table(length, extent):
    phases = frequency(length)[:, None] * np.arange(extent)[None, :] % extent
    angles = phases * (2.0 * np.pi / extent)
    factor = length**0.5 / extent
    cosine, sine = np.cos(angles) * factor, np.sin(angles) * factor
    table = np.stack([np.stack([cosine, sine], 1), np.stack([-sine, cosine], 1)], 0)
    return table.astype(np.float32)


def contract(form, left, right, precision=lax.Precision.HIGHEST):
    return jnp.einsum(form, left, right, precision=precision)


def exchange_slab(rows):
    shape = rows.shape
    packed = rows.reshape(-1, 1, LANES)
    arrived = lax.all_to_all(packed, "slab", 0, 0, tiled=True)
    return arrived.reshape(shape)


def sum_in_order(own, axis):
    index = lax.axis_index(axis)
    one_back = lax.ppermute(own, axis, [(0, 1), (1, 2), (2, 0)])
    two_back = lax.ppermute(own, axis, [(0, 2), (1, 0), (2, 1)])
    first = jnp.where(index == 2, two_back, jnp.where(index == 1, one_back, own))
    second = jnp.where(index == 2, one_back, jnp.where(index == 1, own, two_back))
    third = jnp.where(index == 2, own, jnp.where(index == 1, two_back, one_back))
    return (first + second) + third


def packed_rows(flat):
    members = lax.axis_size("y")
    dense = flat.reshape(-1, LANES)
    each = -(-dense.shape[0] // (members * 8)) * 8
    return jnp.pad(dense, ((0, members * each - dense.shape[0]), (0, 0)))


def shards(coefficients, occupation, pencil_reach, external):
    nbands, planes, width, doubled = coefficients.shape
    points = 2 * width
    slabs = lax.axis_size("slab")
    layers = points // slabs
    part = layers // HALVES
    groups = lax.axis_size("zh") * lax.axis_size("y")
    inverse = inverse_table(width, points)
    forward = forward_table(width, points)
    waves = frequency(width)
    weights = occupation.astype(jnp.float32) / (nbands * groups)

    reach2 = np.abs(np.concatenate([waves, waves])).astype(np.int32)
    sphere = (reach2[None, None, :] <= pencil_reach[:, :, None]).astype(jnp.float32)
    masked = coefficients * sphere[None]
    flat_masked = masked.reshape(nbands * planes * width, doubled)

    def by_half(table, axis):
        shape = table.shape
        return table.reshape(*shape[:axis], slabs, HALVES, part, *shape[axis + 1 :])

    inverse_z = by_half(inverse, 1).transpose(2, 1, 3, 0, 4, 5)
    inverse_z = inverse_z.reshape(HALVES, slabs * part * 2, doubled)
    forward_z = by_half(forward, 3).transpose(4, 3, 5, 2, 0, 1)
    forward_z = forward_z.reshape(HALVES, slabs * part * 2, doubled)
    ext = external.transpose(1, 0, 2).reshape(HALVES, part * points, points)
    member = lax.axis_index("y")

    outgoing = [contract("nk,rk->nr", inverse_z[h], flat_masked) for h in range(HALVES)]
    arrived = []
    for h in range(HALVES):
        rows = outgoing[h].reshape(slabs, part * 2 * nbands * planes * width)
        with jax.named_scope(f"inward{h}"):
            arrived.append(exchange_slab(rows))

    fields, partials = [], []
    for h in range(HALVES):
        if h > 0:
            arrived[h], _ = lax.optimization_barrier((arrived[h], partials[h - 1]))
        blocks = arrived[h].reshape(slabs, part, 2, nbands, planes, width)
        columns = blocks.transpose(3, 0, 4, 1, 2, 5).reshape(nbands, width, part, 2, width)
        spread = contract("bkzcg,oycg->bkzoy", columns, inverse)
        field = contract("bkzcy,oxck->bxzoy", spread, inverse, lax.Precision.HIGH)
        fields.append(field)
        squares = jnp.sum(field * field, axis=3)
        total = sum(weights[b] * squares[b] for b in range(nbands))
        partials.append(packed_rows(total.transpose(1, 0, 2).reshape(part * points, points)))

    potentials = []
    for h in range(HALVES):
        packed = partials[h]
        each = packed.shape[0] // lax.axis_size("y")
        blocks = packed.reshape(-1, each, LANES)
        own = jnp.sum(lax.all_to_all(blocks, "y", 0, 0, tiled=True), axis=0)
        with jax.named_scope(f"across{h}"):
            density = sum_in_order(own, "zh")
        own_external = lax.dynamic_slice_in_dim(packed_rows(ext[h]), member * each, each, 0)
        own_potential = own_external - SLATER * jnp.cbrt(density)
        copies = jnp.broadcast_to(own_potential[None], blocks.shape)
        gathered = lax.all_to_all(copies, "y", 0, 0, tiled=True).reshape(-1, LANES)
        gathered = gathered[: part * points * points // LANES]
        potentials.append(gathered.reshape(part, points, points))

    returned = 0.0
    for h in range(HALVES):
        local = potentials[h].transpose(1, 0, 2)
        product = fields[h] * local[None, :, :, None, :]
        back_x = contract("bxzcy,okcx->bkzoy", product, forward, lax.Precision.HIGH)
        back_y = contract("bkzcy,ogcy->bkzog", back_x, forward)
        blocks = back_y.reshape(nbands, slabs, planes, part, 2, width)
        rows = blocks.transpose(1, 3, 4, 0, 2, 5).reshape(slabs, -1)
        with jax.named_scope(f"outward{h}"):
            home = exchange_slab(rows)
        home = home.reshape(slabs * part * 2, nbands * planes * width)
        returned = returned + contract("nr,nk->rk", home, forward_z[h])

    plane_index = lax.axis_index("slab") * planes + jnp.arange(planes, dtype=jnp.int32)
    plane_freq = jnp.where(plane_index < width // 2, plane_index, plane_index - width)
    plane_sq = (plane_freq * plane_freq).astype(jnp.float32)
    wave_sq = (waves * waves).astype(np.float32)
    both_sq = np.concatenate([wave_sq, wave_sq])
    kinetic = KINETIC * (plane_sq[:, None, None] + wave_sq[None, :, None] + both_sq[None, None, :])
    returned = returned.reshape(nbands, planes, width, doubled)
    applied = sphere[None] * (kinetic[None] * masked + returned)
    potential = jnp.concatenate(potentials, axis=0).transpose(1, 0, 2)
    return applied, potential


def solution(mesh):
    finer = Mesh(mesh.devices.reshape(3, 8, mesh.shape["slab"]), ("zh", "y", "slab"))
    return jax.shard_map(
        shards,
        mesh=finer,
        in_specs=(P(BAND, "slab", None, None), P(BAND), P("slab", None), P(None, "slab", None)),
        out_specs=(P(BAND, "slab", None, None), P(None, "slab", None)),
        check_vma=False,
    )
```

```python
import jax
import jax.numpy as jnp
import numpy as np
from jax import lax
from jax.sharding import Mesh
from jax.sharding import PartitionSpec as P

BAND = ("zh", "y")
KINETIC = 0.0005
SLATER = 0.9847
HALVES = 2
LANES = 128


def frequency(length):
    indices = np.arange(length)
    return np.where(indices < length // 2, indices, indices - length)


def inverse_table(length, extent):
    phases = np.arange(extent)[:, None] * frequency(length)[None, :] % extent
    angles = phases * (2.0 * np.pi / extent)
    factor = length ** (-0.5)
    cosine, sine = np.cos(angles) * factor, np.sin(angles) * factor
    table = np.stack([np.stack([cosine, -sine], 1), np.stack([sine, cosine], 1)], 0)
    return table.astype(np.float32)


def forward_table(length, extent):
    phases = frequency(length)[:, None] * np.arange(extent)[None, :] % extent
    angles = phases * (2.0 * np.pi / extent)
    factor = length**0.5 / extent
    cosine, sine = np.cos(angles) * factor, np.sin(angles) * factor
    table = np.stack([np.stack([cosine, sine], 1), np.stack([-sine, cosine], 1)], 0)
    return table.astype(np.float32)


def contract(form, left, right, precision=lax.Precision.HIGHEST):
    return jnp.einsum(form, left, right, precision=precision)


def exchange_slab(rows):
    shape = rows.shape
    packed = rows.reshape(-1, 1, LANES)
    arrived = lax.all_to_all(packed, "slab", 0, 0, tiled=True)
    return arrived.reshape(shape)


def packed_rows(flat):
    members = lax.axis_size("y")
    dense = flat.reshape(-1, LANES)
    each = -(-dense.shape[0] // (members * 8)) * 8
    return jnp.pad(dense, ((0, members * each - dense.shape[0]), (0, 0)))


def shards(coefficients, occupation, pencil_reach, external):
    nbands, planes, width, doubled = coefficients.shape
    points = 2 * width
    slabs = lax.axis_size("slab")
    layers = points // slabs
    part = layers // HALVES
    groups = lax.axis_size("zh") * lax.axis_size("y")
    inverse = inverse_table(width, points)
    forward = forward_table(width, points)
    waves = frequency(width)
    weights = occupation.astype(jnp.float32) / (nbands * groups)

    reach2 = np.abs(np.concatenate([waves, waves])).astype(np.int32)
    inside = reach2[None, None, :] <= pencil_reach[:, :, None]
    masked = jnp.where(inside[None], coefficients, 0.0)
    flat_masked = masked.reshape(nbands * planes * width, doubled)

    def by_half(table, axis):
        shape = table.shape
        return table.reshape(*shape[:axis], slabs, HALVES, part, *shape[axis + 1 :])

    inverse_z = by_half(inverse, 1).transpose(2, 1, 3, 0, 4, 5)
    inverse_z = inverse_z.reshape(HALVES, slabs * part * 2, doubled)
    forward_z = by_half(forward, 3).transpose(4, 3, 5, 2, 0, 1)
    forward_z = forward_z.reshape(HALVES, slabs * part * 2, doubled)
    ext = external.transpose(1, 0, 2).reshape(HALVES, part * points, points)
    member = lax.axis_index("y")

    outgoing = [contract("nk,rk->nr", inverse_z[h], flat_masked) for h in range(HALVES)]
    arrived = []
    for h in range(HALVES):
        rows = outgoing[h].reshape(slabs, part * 2 * nbands * planes * width)
        with jax.named_scope(f"inward{h}"):
            arrived.append(exchange_slab(rows))

    fields, partials = [], []
    for h in range(HALVES):
        if h > 0:
            arrived[h], _ = lax.optimization_barrier((arrived[h], partials[h - 1]))
        blocks = arrived[h].reshape(slabs, part, 2, nbands, planes, width)
        columns = blocks.transpose(3, 0, 4, 1, 2, 5).reshape(nbands, width, part, 2, width)
        spread = contract("bkzcg,oycg->bkzoy", columns, inverse)
        field = contract("bkzcy,oxck->bxzoy", spread, inverse, lax.Precision.HIGH)
        fields.append(field)
        squares = jnp.sum(field * field, axis=3)
        total = sum(weights[b] * squares[b] for b in range(nbands))
        partials.append(packed_rows(total.transpose(1, 0, 2).reshape(part * points, points)))

    potentials = []
    for h in range(HALVES):
        packed = partials[h]
        each = packed.shape[0] // lax.axis_size("y")
        blocks = packed.reshape(-1, each, LANES)
        own = jnp.sum(lax.all_to_all(blocks, "y", 0, 0, tiled=True), axis=0)
        with jax.named_scope(f"across{h}"):
            density = jnp.sum(lax.all_gather(own, "zh", axis=0), axis=0)
        own_external = lax.dynamic_slice_in_dim(packed_rows(ext[h]), member * each, each, 0)
        own_potential = own_external - SLATER * jnp.cbrt(density)
        copies = jnp.broadcast_to(own_potential[None], blocks.shape)
        gathered = lax.all_to_all(copies, "y", 0, 0, tiled=True).reshape(-1, LANES)
        gathered = gathered[: part * points * points // LANES]
        potentials.append(gathered.reshape(part, points, points))

    returned = 0.0
    for h in range(HALVES):
        local = potentials[h].transpose(1, 0, 2)
        product = fields[h] * local[None, :, :, None, :]
        back_x = contract("bxzcy,okcx->bkzoy", product, forward, lax.Precision.HIGH)
        back_y = contract("bkzcy,ogcy->bkzog", back_x, forward)
        blocks = back_y.reshape(nbands, slabs, planes, part, 2, width)
        rows = blocks.transpose(1, 3, 4, 0, 2, 5).reshape(slabs, -1)
        with jax.named_scope(f"outward{h}"):
            home = exchange_slab(rows)
        home = home.reshape(slabs * part * 2, nbands * planes * width)
        returned = returned + contract("nr,nk->rk", home, forward_z[h])

    plane_index = lax.axis_index("slab") * planes + jnp.arange(planes, dtype=jnp.int32)
    plane_freq = jnp.where(plane_index < width // 2, plane_index, plane_index - width)
    plane_sq = (plane_freq * plane_freq).astype(jnp.float32)
    wave_sq = (waves * waves).astype(np.float32)
    both_sq = np.concatenate([wave_sq, wave_sq])
    kinetic = KINETIC * (plane_sq[:, None, None] + wave_sq[None, :, None] + both_sq[None, None, :])
    returned = returned.reshape(nbands, planes, width, doubled)
    late_reach, late = lax.optimization_barrier((pencil_reach, coefficients))
    inside = reach2[None, None, :] <= late_reach[:, :, None]
    applied = jnp.where(inside[None], kinetic[None] * late + returned, 0.0)
    potential = jnp.concatenate(potentials, axis=0).transpose(1, 0, 2)
    return applied, potential


def solution(mesh):
    finer = Mesh(mesh.devices.reshape(3, 8, mesh.shape["slab"]), ("zh", "y", "slab"))
    return jax.shard_map(
        shards,
        mesh=finer,
        in_specs=(P(BAND, "slab", None, None), P(BAND), P("slab", None), P(None, "slab", None)),
        out_specs=(P(BAND, "slab", None, None), P(None, "slab", None)),
        check_vma=False,
    )
```

```python
import jax
import jax.numpy as jnp
import numpy as np
from jax import lax
from jax.sharding import Mesh
from jax.sharding import PartitionSpec as P

BAND = ("zh", "y")
KINETIC = 0.0005
SLATER = 0.9847
HALVES = 2
LANES = 128


def frequency(length):
    indices = np.arange(length)
    return np.where(indices < length // 2, indices, indices - length)


def inverse_table(length, extent):
    phases = np.arange(extent)[:, None] * frequency(length)[None, :] % extent
    angles = phases * (2.0 * np.pi / extent)
    factor = length ** (-0.5)
    cosine, sine = np.cos(angles) * factor, np.sin(angles) * factor
    table = np.stack([np.stack([cosine, -sine], 1), np.stack([sine, cosine], 1)], 0)
    return table.astype(np.float32)


def forward_table(length, extent):
    phases = frequency(length)[:, None] * np.arange(extent)[None, :] % extent
    angles = phases * (2.0 * np.pi / extent)
    factor = length**0.5 / extent
    cosine, sine = np.cos(angles) * factor, np.sin(angles) * factor
    table = np.stack([np.stack([cosine, sine], 1), np.stack([-sine, cosine], 1)], 0)
    return table.astype(np.float32)


def contract(form, left, right, precision=lax.Precision.HIGHEST):
    return jnp.einsum(form, left, right, precision=precision)


def exchange_slab(rows):
    shape = rows.shape
    packed = rows.reshape(-1, 1, LANES)
    arrived = lax.all_to_all(packed, "slab", 0, 0, tiled=True)
    return arrived.reshape(shape)


def packed_rows(flat):
    members = lax.axis_size("y")
    dense = flat.reshape(-1, LANES)
    each = -(-dense.shape[0] // (members * 8)) * 8
    return jnp.pad(dense, ((0, members * each - dense.shape[0]), (0, 0)))


def shards(coefficients, occupation, pencil_reach, external):
    nbands, planes, width, doubled = coefficients.shape
    points = 2 * width
    slabs = lax.axis_size("slab")
    layers = points // slabs
    part = layers // HALVES
    groups = lax.axis_size("zh") * lax.axis_size("y")
    inverse = inverse_table(width, points)
    forward = forward_table(width, points)
    waves = frequency(width)
    weights = occupation.astype(jnp.float32) / (nbands * groups)

    reach2 = np.abs(np.concatenate([waves, waves])).astype(np.int32)
    inside = reach2[None, None, :] <= pencil_reach[:, :, None]
    masked = jnp.where(inside[None], coefficients, 0.0)
    flat_masked = masked.reshape(nbands * planes * width, doubled)

    def by_half(table, axis):
        shape = table.shape
        return table.reshape(*shape[:axis], slabs, HALVES, part, *shape[axis + 1 :])

    inverse_z = by_half(inverse, 1).transpose(2, 1, 3, 0, 4, 5)
    inverse_z = inverse_z.reshape(HALVES, slabs * part * 2, doubled)
    forward_z = by_half(forward, 3).transpose(4, 3, 5, 2, 0, 1)
    forward_z = forward_z.reshape(HALVES, slabs * part * 2, doubled)
    ext = external.transpose(1, 0, 2).reshape(HALVES, part * points, points)
    member = lax.axis_index("y")

    outgoing = [contract("nk,rk->nr", inverse_z[h], flat_masked) for h in range(HALVES)]
    arrived = []
    for h in range(HALVES):
        rows = outgoing[h].reshape(slabs, part * 2 * nbands * planes * width)
        with jax.named_scope(f"inward{h}"):
            arrived.append(exchange_slab(rows))

    fields, partials = [], []
    for h in range(HALVES):
        if h > 0:
            arrived[h], _ = lax.optimization_barrier((arrived[h], partials[h - 1]))
        blocks = arrived[h].reshape(slabs, part, 2, nbands, planes, width)
        columns = blocks.transpose(3, 0, 4, 1, 2, 5).reshape(nbands, width, part, 2, width)
        spread = contract("bkzcg,oycg->bkzoy", columns, inverse)
        field = contract("bkzcy,oxck->bxzoy", spread, inverse, lax.Precision.HIGH)
        fields.append(field)
        squares = jnp.sum(field * field, axis=3)
        total = sum(weights[b] * squares[b] for b in range(nbands))
        partials.append(packed_rows(total.transpose(1, 0, 2).reshape(part * points, points)))

    potentials = []
    for h in range(HALVES):
        packed = partials[h]
        each = packed.shape[0] // lax.axis_size("y")
        blocks = packed.reshape(-1, each, LANES)
        own = jnp.sum(lax.all_to_all(blocks, "y", 0, 0, tiled=True), axis=0)
        with jax.named_scope(f"across{h}"):
            density = jnp.sum(lax.all_gather(own, "zh", axis=0), axis=0)
        own_external = lax.dynamic_slice_in_dim(packed_rows(ext[h]), member * each, each, 0)
        own_potential = own_external - SLATER * jnp.cbrt(density)
        copies = jnp.broadcast_to(own_potential[None], blocks.shape)
        gathered = lax.all_to_all(copies, "y", 0, 0, tiled=True).reshape(-1, LANES)
        gathered = gathered[: part * points * points // LANES]
        potentials.append(gathered.reshape(part, points, points))

    returned = 0.0
    for h in range(HALVES):
        local = potentials[h].transpose(1, 0, 2)
        product = fields[h] * local[None, :, :, None, :]
        back_x = contract("bxzcy,okcx->bkzoy", product, forward, lax.Precision.HIGH)
        back_y = contract("bkzcy,ogcy->bkzog", back_x, forward)
        blocks = back_y.reshape(nbands, slabs, planes, part, 2, width)
        rows = blocks.transpose(1, 3, 4, 0, 2, 5).reshape(slabs, -1)
        with jax.named_scope(f"outward{h}"):
            home = exchange_slab(rows)
        home = home.reshape(slabs * part * 2, nbands * planes * width)
        returned = returned + contract("nr,nk->rk", home, forward_z[h])

    plane_index = lax.axis_index("slab") * planes + jnp.arange(planes, dtype=jnp.int32)
    plane_freq = jnp.where(plane_index < width // 2, plane_index, plane_index - width)
    plane_sq = (plane_freq * plane_freq).astype(jnp.float32)
    wave_sq = (waves * waves).astype(np.float32)
    both_sq = np.concatenate([wave_sq, wave_sq])
    kinetic = KINETIC * (plane_sq[:, None, None] + wave_sq[None, :, None] + both_sq[None, None, :])
    returned = returned.reshape(nbands, planes, width, doubled)
    late_reach, late, _ = lax.optimization_barrier((pencil_reach, coefficients, potentials[0]))
    inside = reach2[None, None, :] <= late_reach[:, :, None]
    applied = jnp.where(inside[None], kinetic[None] * late + returned, 0.0)
    potential = jnp.concatenate(potentials, axis=0).transpose(1, 0, 2)
    return applied, potential


def solution(mesh):
    finer = Mesh(mesh.devices.reshape(3, 8, mesh.shape["slab"]), ("zh", "y", "slab"))
    return jax.shard_map(
        shards,
        mesh=finer,
        in_specs=(P(BAND, "slab", None, None), P(BAND), P("slab", None), P(None, "slab", None)),
        out_specs=(P(BAND, "slab", None, None), P(None, "slab", None)),
        check_vma=False,
    )
```
